128 devices in a mesh: dp: 16 (over y_hi, x, core), expert: 8 (over z, y_lo).
Axes of the slice: x: 4, y: 4 (y_hi: 2, y_lo: 2; y = y_hi * 2 + y_lo), z: 4, core: 2. Of those that a mesh axis runs over, the one named last changes fastest.
Arguments:
- tokens: bfloat16 [32, 2048, 4096], P('dp', 'expert'), may hold values from -6 to 6
- out_grad: bfloat16 [32, 2048, 4096], P('dp', 'expert'), may hold values from -6 to 6
- router: bfloat16 [4096, 8], replicated, may hold values from -4 to 4
- weight_in: bfloat16 [8, 4096, 512], P('expert', 'dp'), may hold values from -0.09375 to 0.09375
- weight_out: bfloat16 [8, 4096, 512], P('expert', 'dp'), may hold values from -0.25 to 0.25
Outputs:
- token_grad: bfloat16 [32, 2048, 4096], P(None, ('expert', 'dp'))
- grad_in: float32 [8, 4096, 512], P('expert', 'dp')
- grad_out: float32 [8, 4096, 512], P('expert', 'dp')
The draws below stay inside these ranges and needn't reach their ends.
All inputs are finite; a program needn't handle non-finite values.
Results may differ from the reference program's by a relative error of at most 0.022.
Values may be sent and summed in bfloat16 or wider, within the bound.
No kernel may reach another device: no remote copies, remote signals or barrier semaphores. Data moves between devices by JAX's collectives and lax.ppermute only.
A program may use at most 128 MiB of HBM per device.

```python
import jax
import jax.numpy as jnp
from jax import lax

D = 4096
HID = 512
POS_DEV = 16
SEQS = 32
LENGTH = 2048
EXPERTS = 8
N_DP = 16
N_EXPERT = 8


def draw_tokens(key, part):
    local_key = jax.random.fold_in(key, 11)
    sample = jax.random.normal(local_key, (SEQS, LENGTH, D), jnp.float32)
    return jnp.clip(sample, -6.0, 6.0).astype(jnp.bfloat16)


def draw_router(key, part):
    local_key = jax.random.fold_in(key, 13)
    sub_keys = jax.random.split(local_key, 2)
    column_scale = jnp.exp(jax.random.uniform(sub_keys[0], (EXPERTS,), jnp.float32, jnp.log(0.5), jnp.log(3.0)))
    sample = jax.random.normal(sub_keys[1], (D, EXPERTS), jnp.float32) * column_scale[None, :] / jnp.sqrt(1.0 * D)
    return jnp.clip(sample, -4.0, 4.0).astype(jnp.bfloat16)


def shard_levels(own_key, dims, shards, low, largest):
    def one(axis_at, parts):
        steps = jax.random.uniform(jax.random.fold_in(jax.random.fold_in(own_key, 6), axis_at), (parts,), jnp.float32, low / len(shards), largest / len(shards))
        return jnp.repeat(jnp.exp(steps), dims[axis_at] // parts).reshape((-1,) + (1,) * (len(dims) - axis_at - 1))

    loudness = one(*shards[0])
    for cut in shards[1:]:
        loudness = loudness * one(*cut)
    return loudness


def bell_draw(rng, shape, spread, limit, pieces=(), kind=jnp.bfloat16):
    loudness = shard_levels(rng, shape, pieces, -0.22, 0.18) if pieces else 1.0
    values = jax.random.normal(rng, shape, jnp.float32) * spread * loudness
    return jnp.minimum(jnp.maximum(values, -limit), limit).astype(kind)


def setup_inputs(seed: int = 0) -> dict:
    streams_of = jax.random.split(jax.random.key(seed), 6)
    return {
        "tokens": draw_tokens(jax.random.fold_in(streams_of[5], 71), 0),
        "out_grad": bell_draw(streams_of[1], (SEQS, LENGTH, D), 1.0, 6.0, ((0, 16), (1, 8))),
        "router": draw_router(jax.random.fold_in(streams_of[5], 71), 0),
        "weight_in": bell_draw(streams_of[3], (EXPERTS, D, HID), D ** -0.5, 0.09375, ((0, 8), (1, 16))),
        "weight_out": bell_draw(streams_of[4], (EXPERTS, D, HID), HID ** -0.5, 0.25, ((0, 8), (1, 16))),
    }


def reference(tokens, out_grad, router, weight_in, weight_out):
    router_wide = router.astype(jnp.float32)
    inner_weights = weight_in.astype(jnp.float32)
    outer_weights = weight_out.astype(jnp.float32)

    def outer_step(running, dp_index):
        def inner_step(partial_value, expert_index):
            first_pos = ((expert_index * N_DP + dp_index) * POS_DEV).astype(jnp.int32)
            block_tokens = lax.dynamic_slice_in_dim(tokens, first_pos, POS_DEV, 1).astype(jnp.float32)
            block_grads = lax.dynamic_slice_in_dim(out_grad, first_pos, POS_DEV, 1).astype(jnp.float32)
            logits = jnp.einsum('spd,de->spe', block_tokens, router_wide)
            probs = jax.nn.softmax(logits, axis=0)
            mixing = probs.astype(jnp.bfloat16).astype(jnp.float32)
            mixed = jnp.einsum('spe,spd->epd', mixing, block_tokens).astype(jnp.bfloat16).astype(jnp.float32)
            mixed_grad = jnp.einsum('spe,spd->epd', mixing, block_grads).astype(jnp.bfloat16).astype(jnp.float32)
            pre = jnp.einsum('epd,edh->eph', mixed, inner_weights)
            sigma = jax.nn.sigmoid(pre)
            hidden = (pre * sigma).astype(jnp.bfloat16).astype(jnp.float32)
            expert_out = jnp.einsum('eph,edh->epd', hidden, outer_weights).astype(jnp.bfloat16).astype(jnp.float32)
            hidden_full = jnp.einsum('epd,edh->eph', mixed_grad, outer_weights)
            hidden_grad = (hidden_full * sigma * (1.0 + pre * (1.0 - sigma))).astype(jnp.bfloat16).astype(jnp.float32)
            input_grad = jnp.einsum('eph,edh->epd', hidden_grad, inner_weights).astype(jnp.bfloat16).astype(jnp.float32)
            grad_in_part = jnp.einsum('epd,eph->edh', mixed, hidden_grad)
            grad_out_part = jnp.einsum('epd,eph->edh', mixed_grad, hidden)
            weight_grad = jnp.einsum('spd,epd->spe', block_grads, expert_out) + jnp.einsum('spd,epd->spe', block_tokens, input_grad)
            logit_grad = probs * (weight_grad - jnp.sum(probs * weight_grad, axis=0, keepdims=True))
            logit_round = logit_grad.astype(jnp.bfloat16).astype(jnp.float32)
            block_out = jnp.einsum('spe,epd->spd', mixing, input_grad) + jnp.einsum('spe,de->spd', logit_round, router_wide)
            return (partial_value[0] + grad_in_part, partial_value[1] + grad_out_part), block_out.astype(jnp.bfloat16)

        empty_grads = (jnp.zeros((EXPERTS, D, HID), jnp.float32), jnp.zeros((EXPERTS, D, HID), jnp.float32))
        inner_sums, block_grads_all = lax.scan(inner_step, empty_grads, jnp.arange(N_EXPERT, dtype=jnp.int32))
        rounded_in = lax.optimization_barrier(inner_sums[0].astype(jnp.bfloat16)).astype(jnp.float32)
        rounded_out = lax.optimization_barrier(inner_sums[1].astype(jnp.bfloat16)).astype(jnp.float32)
        return (running[0] + rounded_in, running[1] + rounded_out), block_grads_all

    start_grads = (jnp.zeros((EXPERTS, D, HID), jnp.float32), jnp.zeros((EXPERTS, D, HID), jnp.float32))
    sums_all, block_grads = lax.scan(outer_step, start_grads, jnp.arange(N_DP, dtype=jnp.int32))
    token_grad = jnp.transpose(block_grads, (2, 1, 0, 3, 4)).reshape(SEQS, N_EXPERT * N_DP * POS_DEV, D)
    return token_grad, sums_all[0], sums_all[1]
```

```python
import functools

import jax
import jax.numpy as jnp
from jax import lax
from jax.experimental import pallas as pl
from jax.experimental.pallas import tpu as pltpu
from jax.sharding import Mesh
from jax.sharding import PartitionSpec as P

BF = jnp.bfloat16
F32 = jnp.float32
D = 4096
HALF = 2048
HID = 512
SEQS = 32
EXPERTS = 8
POS = 16
ROWS = SEQS * POS
LANES = EXPERTS * POS
SHARD = 256
MIB = 1024 * 1024
VM = pl.BlockSpec(memory_space=pltpu.VMEM)


def call(kernel, outs, n_in, name, flops, nbytes, scalars=0, scratch=()):
    return pl.pallas_call(
        kernel,
        out_shape=outs,
        grid_spec=pltpu.PrefetchScalarGridSpec(
            num_scalar_prefetch=scalars,
            in_specs=[VM] * n_in,
            out_specs=jax.tree.map(lambda _: VM, outs),
            scratch_shapes=scratch,
        ),
        compiler_params=pltpu.CompilerParams(vmem_limit_bytes=48 * MIB),
        cost_estimate=pl.CostEstimate(flops=flops, bytes_accessed=nbytes, transcendentals=0),
        name=name,
    )


def shape(dims, dtype):
    return jax.ShapeDtypeStruct(dims, dtype)


def nt(a, b):
    return lax.dot_general(a, b, (((1,), (1,)), ((), ())), preferred_element_type=F32)


def tn(a, b):
    return lax.dot_general(a, b, (((0,), (0,)), ((), ())), preferred_element_type=F32)


def pack_kernel(t_ref, g_ref, o_ref):
    o_ref[0, 0:2] = t_ref[...]
    o_ref[0, 2:4] = g_ref[...]


def pack(tokens, out_grad):
    rows = pl.BlockSpec((2, POS, D), lambda j: (0, j, 0))
    return pl.pallas_call(
        pack_kernel,
        out_shape=shape((16, 4, POS, D), BF),
        grid=(16,),
        in_specs=[rows, rows],
        out_specs=pl.BlockSpec((1, 4, POS, D), lambda j: (j, 0, 0, 0)),
        cost_estimate=pl.CostEstimate(flops=8 * MIB, bytes_accessed=16 * MIB, transcendentals=0),
        name="pack",
    )(tokens, out_grad)


def own_position():
    row = lax.broadcasted_iota(jnp.int32, (POS, LANES), 0)
    lane = lax.broadcasted_iota(jnp.int32, (POS, LANES), 1)
    return (lane % POS == row)[None]


def mix_kernel(a_ref, rxt_ref, f_ref, probs_ref, mixing_ref):
    logits = jnp.zeros((ROWS, LANES), F32)
    for j in range(4):
        cols = pl.ds(j * 1024, 1024)
        logits += nt(a_ref[:, 0:2, :, cols].reshape(ROWS, 1024), rxt_ref[:, cols])
    logits = logits.reshape(SEQS, POS, LANES)
    weights = jnp.exp(logits - jnp.max(logits, axis=0, keepdims=True))
    probs = weights / jnp.sum(weights, axis=0, keepdims=True)
    probs = jnp.where(own_position(), probs, 0.0).reshape(ROWS, LANES)
    probs_ref[...] = probs
    mixing_ref[...] = probs.astype(BF)
    mixing_t = probs.T.astype(BF)
    for j in range(8):
        cols = pl.ds(j * 512, 512)
        half, part = j // 4, pl.ds(j % 4 * 512, 512)
        for t in range(2):
            block = a_ref[:, 2 * t : 2 * t + 2, :, cols].reshape(ROWS, 512)
            mixed = jnp.dot(mixing_t, block, preferred_element_type=F32)
            f_ref[half, :, t, :, part] = mixed.astype(BF).reshape(EXPERTS, POS, 512)


def shard_columns(dev_ref, k, j):
    owner = lax.rem(dev_ref[0] + 4 - k, 4) * 2 + lax.rem(dev_ref[1] + j, 2)
    return pl.ds(pl.multiple_of(owner * SHARD, SHARD), SHARD)


def partial_kernel(dev_ref, f_ref, *refs):
    w_refs, (own_ref, send_ref) = refs[:8], refs[8:]
    sums = [jnp.zeros((256, HID), F32) for _ in range(2)]
    for k in range(4):
        for j in range(2):
            cols = shard_columns(dev_ref, k, j)
            for t in range(2):
                block = f_ref[:, t, :, cols].reshape(256, SHARD)
                sums[t] += jnp.dot(block, w_refs[2 * k + j][t], preferred_element_type=F32)
    for t in range(2):
        own_ref[t] = sums[t]
        send_ref[t] = sums[t].astype(BF)


def expert_kernel(dev_ref, own_ref, other_ref, *refs):
    w_refs, (b_ref, hidden_ref) = refs[:8], refs[8:]
    pre = own_ref[0] + other_ref[0].astype(F32)
    hidden_full = own_ref[1] + other_ref[1].astype(F32)
    sigma = jax.nn.sigmoid(pre)
    hidden = (pre * sigma).astype(BF)
    hidden_grad = (hidden_full * sigma * (1.0 + pre * (1.0 - sigma))).astype(BF)
    hidden_ref[0] = hidden_grad
    hidden_ref[1] = hidden
    for k in range(4):
        for j in range(2):
            cols = shard_columns(dev_ref, k, j)
            w_ref = w_refs[2 * k + j]
            b_ref[:, 0, :, cols] = nt(hidden, w_ref[1]).astype(BF).reshape(16, POS, SHARD)
            b_ref[:, 1, :, cols] = nt(hidden_grad, w_ref[0]).astype(BF).reshape(16, POS, SHARD)


def grads_kernel(dev_ref, f_ref, hidden_ref, keep_ref, send_ref):
    for k in range(4):
        for j, out_ref in enumerate((keep_ref, send_ref)):
            owner = lax.rem(dev_ref[0] + k, 4) * 2 + lax.rem(dev_ref[1] + j, 2)
            cols = pl.ds(pl.multiple_of(owner * SHARD, SHARD), SHARD)
            for t in range(2):
                block = f_ref[:, t, :, cols].reshape(256, SHARD)
                out_ref[k, t] = tn(block, hidden_ref[t]).astype(BF)


def add_kernel(keep_ref, got_ref, own_ref, *send_refs):
    own_ref[...] = keep_ref[0].astype(F32) + got_ref[0].astype(F32)
    for k in range(1, 4):
        total = keep_ref[k].astype(F32) + got_ref[k].astype(F32)
        send_refs[k - 1][...] = total.astype(BF)


def sum_kernel(own_ref, a_ref, b_ref, c_ref, in_ref, out_ref):
    for t, ref in enumerate((in_ref, out_ref)):
        ref[...] = own_ref[t] + a_ref[t].astype(F32) + b_ref[t].astype(F32) + c_ref[t].astype(F32)


def final_kernel(a_ref, b_ref, rxt_ref, probs_ref, mixing_ref, o_ref):
    weight_grad = jnp.zeros((ROWS, LANES), F32)
    for j in range(8):
        cols = pl.ds(j * 512, 512)
        half, part = pl.ds(j // 4 * EXPERTS, EXPERTS), pl.ds(j % 4 * 512, 512)
        for t in range(2):
            block = a_ref[:, 2 - 2 * t : 4 - 2 * t, :, cols].reshape(ROWS, 512)
            weight_grad += nt(block, b_ref[half, t, :, part].reshape(LANES, 512))
    probs = probs_ref[...].reshape(SEQS, POS, LANES)
    weight_grad = weight_grad.reshape(SEQS, POS, LANES)
    mean = jnp.sum(probs * weight_grad, axis=0, keepdims=True)
    logit_grad = (probs * (weight_grad - mean)).reshape(ROWS, LANES).astype(BF)
    both = jnp.concatenate([mixing_ref[...], logit_grad], axis=1)
    for j in range(8):
        cols = pl.ds(j * 512, 512)
        half, part = pl.ds(j // 4 * EXPERTS, EXPERTS), pl.ds(j % 4 * 512, 512)
        right = jnp.concatenate([b_ref[half, 1, :, part].reshape(LANES, 512), rxt_ref[:, cols]], axis=0)
        out = jnp.dot(both, right, preferred_element_type=F32)
        o_ref[:, :, cols] = out.astype(BF).reshape(SEQS, POS, 512)


def shift(x, k):
    return lax.ppermute(x, "x", [(i, (i + k) % 4) for i in range(4)])


def swap(x, axis):
    return lax.ppermute(x, axis, [(0, 1), (1, 0)])


def on_device(tokens, out_grad, router, weight_in, weight_out):
    dev = jnp.stack([lax.axis_index("x"), lax.axis_index("c")]).astype(jnp.int32)
    rxt = jnp.repeat(router.T, POS, axis=0)
    shard = jnp.concatenate([weight_in, weight_out], axis=0)

    rows = lax.all_to_all(pack(tokens, out_grad), ("yh", "x", "c"), 0, 0, tiled=True)
    mixed, probs, mixing = call(
        mix_kernel,
        (shape((2, EXPERTS, 2, POS, HALF), BF), shape((ROWS, LANES), F32), shape((ROWS, LANES), BF)),
        2, "mix", 3 * 10**9, 12 * MIB,
    )(rows, rxt)

    experts = ("yh", "z", "yl")
    got = lax.all_to_all(mixed.reshape(16, 2, POS, HALF), experts, 0, 0, tiled=True)

    shard, _ = lax.optimization_barrier((shard, mixing))
    shards = [shard] + [shift(shard, k) for k in range(1, 4)]
    weights = []
    for w in shards:
        weights += [w, swap(w, "c")]

    own, send = call(
        partial_kernel,
        (shape((2, 256, HID), F32), shape((2, 256, HID), BF)),
        9, "partial", 10**9, 8 * MIB, scalars=1,
    )(dev, got, *weights)
    other = swap(send, "yh")
    back, hidden = call(
        expert_kernel,
        (shape((16, 2, POS, HALF), BF), shape((2, 256, HID), BF)),
        10, "expert", 10**9, 8 * MIB, scalars=1,
    )(dev, own, other, *weights)
    back = lax.all_to_all(back, experts, 0, 0, tiled=True)

    keep, cross = call(
        grads_kernel,
        (shape((4, 2, SHARD, HID), BF), shape((4, 2, SHARD, HID), BF)),
        2, "grads", 10**9, 8 * MIB, scalars=1,
    )(dev, got, hidden)
    cross = swap(cross, "c")
    piece = shape((2, SHARD, HID), BF)
    own_sum, *sends = call(
        add_kernel, (shape((2, SHARD, HID), F32), piece, piece, piece), 2, "add", 10**7, 8 * MIB,
    )(keep, cross)
    sums = [shift(s, k) for k, s in enumerate(sends, 1)]
    grad_in, grad_out = call(
        sum_kernel, (shape((SHARD, HID), F32), shape((SHARD, HID), F32)), 4, "sum", 10**7, 4 * MIB,
    )(own_sum, *sums)

    token_grad = call(
        final_kernel, shape((SEQS, POS, D), BF), 5, "final", 4 * 10**9, 16 * MIB,
    )(rows, back, rxt, probs, mixing)
    return token_grad, grad_in[None], grad_out[None]


def solution(mesh):
    fine = Mesh(mesh.devices.reshape(2, 4, 2, 4, 2), ("yh", "x", "c", "z", "yl"))
    dp, expert = ("yh", "x", "c"), ("z", "yl")
    seqs, weights = P(dp, expert, None), P(expert, dp, None)
    return jax.shard_map(
        on_device,
        mesh=fine,
        in_specs=(seqs, seqs, P(), weights, weights),
        out_specs=(P(None, expert + dp, None), weights, weights),
        check_vma=False,
    )
```

```python
import jax
import jax.numpy as jnp
from jax import lax
from jax.experimental import pallas as pl
from jax.experimental.pallas import tpu as pltpu
from jax.sharding import Mesh
from jax.sharding import PartitionSpec as P

BF = jnp.bfloat16
F32 = jnp.float32
D = 4096
HALF = 2048
HID = 512
SEQS = 32
EXPERTS = 8
POS = 16
ROWS = SEQS * POS
LANES = EXPERTS * POS
SHARD = 256
MIB = 1024 * 1024
ORDER = (2, 1, 3, 0)
VM = pl.BlockSpec(memory_space=pltpu.VMEM)
HBM = pl.BlockSpec(memory_space=pltpu.HBM)


def call(kernel, outs, n_in, flops, nbytes, vmem, scratch=(), specs=None, far=0):
    return pl.pallas_call(
        kernel,
        out_shape=outs,
        in_specs=[VM] * n_in + [HBM] * far,
        out_specs=specs or jax.tree.map(lambda _: VM, outs),
        scratch_shapes=scratch,
        compiler_params=pltpu.CompilerParams(vmem_limit_bytes=vmem * MIB),
        cost_estimate=pl.CostEstimate(flops=flops, bytes_accessed=nbytes, transcendentals=0),
    )


def shape(dims, dtype):
    return jax.ShapeDtypeStruct(dims, dtype)


def in_hbm(x):
    return pltpu.with_memory_space_constraint(x, pltpu.HBM)


def nt(a, b):
    return lax.dot_general(a, b, (((1,), (1,)), ((), ())), preferred_element_type=F32)


def tn(a, b):
    return lax.dot_general(a, b, (((0,), (0,)), ((), ())), preferred_element_type=F32)


def pack_kernel(t_ref, g_ref, wi_ref, wo_ref, router_ref, o_ref, w_ref, rxt_ref, sem):
    copies = []
    for i in range(16):
        src, seq, part = (t_ref, g_ref)[i // 8], i // 4 % 2, pl.ds(i % 4 * 4, 4)
        copies.append(pltpu.make_async_copy(src.at[seq, part], o_ref.at[part, i // 4], sem.at[i]))
    copies.append(pltpu.make_async_copy(wi_ref.at[0], w_ref.at[0], sem.at[16]))
    copies.append(pltpu.make_async_copy(wo_ref.at[0], w_ref.at[1], sem.at[17]))
    for copy in copies:
        copy.start()
    for e in range(EXPERTS):
        row = router_ref[e : e + 1, :].astype(F32)
        rxt_ref[e * POS : (e + 1) * POS, :] = jnp.broadcast_to(row, (POS, D)).astype(BF)
    for copy in copies:
        copy.wait()


def pack(tokens, out_grad, weight_in, weight_out, router):
    blocks = (2, 16, POS, D)
    arrays = (tokens.reshape(blocks), out_grad.reshape(blocks), weight_in, weight_out)
    return pl.pallas_call(
        pack_kernel,
        out_shape=(shape((16, 4, POS, D), BF), shape((2, SHARD, HID), BF), shape((LANES, D), BF)),
        in_specs=[HBM] * 4 + [VM],
        out_specs=(VM, VM, VM),
        scratch_shapes=[pltpu.SemaphoreType.DMA((18,))],
        cost_estimate=pl.CostEstimate(flops=8 * MIB, bytes_accessed=16 * MIB, transcendentals=0),
        compiler_params=pltpu.CompilerParams(vmem_limit_bytes=16 * MIB),
        name="pack",
    )(*[in_hbm(a) for a in arrays], router.T)


def own_position():
    row = lax.broadcasted_iota(jnp.int32, (POS, LANES), 0)
    lane = lax.broadcasted_iota(jnp.int32, (POS, LANES), 1)
    return (lane % POS == row)[None]


def mix_kernel(a_ref, rxt_ref, f_ref, probs_ref, mixing_ref, held, sem):
    logits = jnp.zeros((LANES, ROWS), F32)
    for j in range(4):
        cols = pl.ds(j * 1024, 1024)
        logits += nt(rxt_ref[:, cols], a_ref[:, 0:2, :, cols].reshape(ROWS, 1024))
    logits = logits.T.reshape(SEQS, POS, LANES)
    weights = jnp.exp(logits - jnp.max(logits, axis=0, keepdims=True))
    probs = weights / jnp.sum(weights, axis=0, keepdims=True)
    probs = jnp.where(own_position(), probs, 0.0).reshape(ROWS, LANES)
    probs_ref[...] = probs
    mixing_ref[...] = probs.astype(BF)
    mixing_t = probs.T.astype(BF)
    copies = []
    for j in range(8):
        cols = pl.ds(j * 512, 512)
        half, part = j // 4, pl.ds(j % 4 * 512, 512)
        for t in range(2):
            block = a_ref[:, 2 * t : 2 * t + 2, :, cols].reshape(ROWS, 512)
            mixed = jnp.dot(mixing_t, block, preferred_element_type=F32)
            held[half, :, t, :, part] = mixed.astype(BF).reshape(EXPERTS, POS, 512)
        place = (half, slice(None), slice(None), slice(None), part)
        copies.append(pltpu.make_async_copy(held.at[place], f_ref.at[place], sem.at[j]))
        copies[j].start()
    for copy in copies:
        copy.wait()


def shard_columns(k, j):
    owner = lax.rem(lax.axis_index("x") + 4 - k, 4) * 2 + lax.rem(lax.axis_index("c") + j, 2)
    return pl.ds(pl.multiple_of(owner * SHARD, SHARD), SHARD)


def partial_kernel(f_ref, *refs):
    shard_refs, (own_ref, send_ref, w_ref, sem) = refs[:8], refs[8:]
    copies = [pltpu.make_async_copy(ref, w_ref.at[i], sem.at[i]) for i, ref in enumerate(shard_refs)]
    for copy in copies:
        copy.start()
    sums = [jnp.zeros((256, HID), F32) for _ in range(2)]
    for i, copy in enumerate(copies):
        cols = shard_columns(i // 2, i % 2)
        copy.wait()
        for t in range(2):
            block = f_ref[:, t, :, cols].reshape(256, SHARD)
            sums[t] += jnp.dot(block, w_ref[i, t], preferred_element_type=F32)
    for t in range(2):
        own_ref[t] = sums[t]
        send_ref[t] = sums[t].astype(BF)


def expert_kernel(own_ref, other_ref, w_ref, b_ref, hidden_ref, held, sem):
    pre = own_ref[0] + other_ref[0].astype(F32)
    hidden_full = own_ref[1] + other_ref[1].astype(F32)
    sigma = jax.nn.sigmoid(pre)
    hidden = (pre * sigma).astype(BF)
    hidden_grad = (hidden_full * sigma * (1.0 + pre * (1.0 - sigma))).astype(BF)
    hidden_ref[0] = hidden_grad
    hidden_ref[1] = hidden
    copies = []
    for i in range(8):
        cols = shard_columns(i // 2, i % 2)
        held[:, 0, :, cols] = nt(hidden, w_ref[i, 1]).astype(BF).reshape(16, POS, SHARD)
        held[:, 1, :, cols] = nt(hidden_grad, w_ref[i, 0]).astype(BF).reshape(16, POS, SHARD)
        place = (slice(None), slice(None), slice(None), cols)
        copies.append(pltpu.make_async_copy(held.at[place], b_ref.at[place], sem.at[i]))
        copies[i].start()
    for copy in copies:
        copy.wait()


def grads_kernel(f_ref, hidden_ref, *out_refs):
    for n, k in enumerate(ORDER):
        for j in range(2):
            cols = shard_columns(4 - k, j)
            for t in range(2):
                block = f_ref[:, t, :, cols].reshape(256, SHARD)
                out_refs[2 * n + j][t] = tn(block, hidden_ref[t]).astype(BF)


def add_kernel(keep_ref, got_ref, o_ref):
    o_ref[...] = (keep_ref[...].astype(F32) + got_ref[...].astype(F32)).astype(o_ref.dtype)


def sum_kernel(own_ref, a_ref, b_ref, c_ref, in_ref, out_ref):
    for t, ref in enumerate((in_ref, out_ref)):
        ref[0] = own_ref[t] + a_ref[t].astype(F32) + b_ref[t].astype(F32) + c_ref[t].astype(F32)


def final_kernel(b_ref, probs_ref, mixing_ref, rows_ref, far_rxt_ref, o_ref, a_ref, rxt_ref, held, in_sem, sem):
    reads = []
    for j in range(8):
        cols = pl.ds(j * 512, 512)
        reads.append(pltpu.make_async_copy(rows_ref.at[..., cols], a_ref.at[..., cols], in_sem.at[j]))
    reads.append(pltpu.make_async_copy(far_rxt_ref, rxt_ref, in_sem.at[8]))
    for copy in reads:
        copy.start()
    weight_grad = jnp.zeros((LANES, ROWS), F32)
    for j in range(8):
        cols = pl.ds(j * 512, 512)
        reads[j].wait()
        half, part = pl.ds(j // 4 * EXPERTS, EXPERTS), pl.ds(j % 4 * 512, 512)
        for t in range(2):
            block = a_ref[:, 2 - 2 * t : 4 - 2 * t, :, cols].reshape(ROWS, 512)
            weight_grad += nt(b_ref[half, t, :, part].reshape(LANES, 512), block)
    probs = probs_ref[...].reshape(SEQS, POS, LANES)
    weight_grad = weight_grad.T.reshape(SEQS, POS, LANES)
    mean = jnp.sum(probs * weight_grad, axis=0, keepdims=True)
    logit_grad = (probs * (weight_grad - mean)).reshape(ROWS, LANES).astype(BF)
    both = jnp.concatenate([mixing_ref[...], logit_grad], axis=1)
    reads[8].wait()
    copies = []
    for j in range(8):
        cols = pl.ds(j * 512, 512)
        half, part = pl.ds(j // 4 * EXPERTS, EXPERTS), pl.ds(j % 4 * 512, 512)
        right = jnp.concatenate([b_ref[half, 1, :, part].reshape(LANES, 512), rxt_ref[:, cols]], axis=0)
        out = jnp.dot(both, right, preferred_element_type=F32)
        held[:, :, cols] = out.astype(BF).reshape(SEQS, POS, 512)
        copies.append(pltpu.make_async_copy(held.at[:, :, cols], o_ref.at[:, :, cols], sem.at[j]))
        copies[j].start()
    for copy in copies:
        copy.wait()


def shift(x, k):
    return lax.ppermute(x, "x", [(i, (i + k) % 4) for i in range(4)])


def swap(x, axis):
    return lax.ppermute(x, axis, [(0, 1), (1, 0)])


def on_device(tokens, out_grad, router, weight_in, weight_out):
    rows, shard, rxt = pack(tokens, out_grad, weight_in, weight_out, router)
    rows = lax.all_to_all(rows, ("yh", "x", "c"), 0, 0, tiled=True)
    mixed, probs, mixing = call(
        mix_kernel,
        (pltpu.HBM((2, EXPERTS, 2, POS, HALF), BF), shape((ROWS, LANES), F32), shape((ROWS, LANES), BF)),
        2, 3 * 10**9, 12 * MIB, 22, specs=(HBM, VM, VM),
        scratch=[pltpu.VMEM((2, EXPERTS, 2, POS, HALF), BF), pltpu.SemaphoreType.DMA((8,))],
    )(rows, rxt)

    experts = ("yh", "z", "yl")
    got = lax.all_to_all(mixed.reshape(16, 2, POS, HALF), experts, 0, 0, tiled=True)

    shard, _ = lax.optimization_barrier((shard, mixing))
    shards = [shard] + [shift(shard, k) for k in range(1, 4)]
    weights = []
    for w in shards:
        weights += [w, swap(w, "c")]

    own, send, weights = call(
        partial_kernel,
        (shape((2, 256, HID), F32), shape((2, 256, HID), BF), shape((8, 2, SHARD, HID), BF)),
        1, 10**9, 8 * MIB, 14, far=8,
        scratch=[pltpu.SemaphoreType.DMA((8,))],
    )(got, *[in_hbm(w) for w in weights])
    other = swap(send, "yh")
    back, hidden = call(
        expert_kernel,
        (pltpu.HBM((16, 2, POS, HALF), BF), shape((2, 256, HID), BF)),
        3, 10**9, 8 * MIB, 16, specs=(HBM, VM),
        scratch=[pltpu.VMEM((16, 2, POS, HALF), BF), pltpu.SemaphoreType.DMA((8,))],
    )(own, other, weights)
    back = lax.all_to_all(back, experts, 0, 0, tiled=True)

    piece = shape((2, SHARD, HID), BF)
    parts = call(grads_kernel, (piece,) * 8, 2, 10**9, 8 * MIB, 14)(got, hidden)
    sums = []
    for n, k in enumerate(ORDER):
        got_part = swap(parts[2 * n + 1], "c")
        total = shape((2, SHARD, HID), BF if k else F32)
        total = call(add_kernel, total, 2, 10**6, 2 * MIB, 4)(parts[2 * n], got_part)
        sums.append(shift(total, k) if k else total)
    token_grad = call(
        final_kernel, shape((SEQS, POS, D), BF), 3, 4 * 10**9, 16 * MIB, 32, specs=HBM, far=2,
        scratch=[
            pltpu.VMEM((16, 4, POS, D), BF),
            pltpu.VMEM((LANES, D), BF),
            pltpu.VMEM((SEQS, POS, D), BF),
            pltpu.SemaphoreType.DMA((9,)),
            pltpu.SemaphoreType.DMA((8,)),
        ],
    )(back, probs, mixing, in_hbm(rows), in_hbm(rxt))
    token_grad, *sums = lax.optimization_barrier((token_grad, *sums))
    grad = shape((1, SHARD, HID), F32)
    grad_in, grad_out = call(sum_kernel, (grad, grad), 4, 10**6, 4 * MIB, 6)(
        sums[3], sums[0], sums[1], sums[2]
    )
    return token_grad, grad_in, grad_out


def solution(mesh):
    fine = Mesh(mesh.devices.reshape(2, 4, 2, 4, 2), ("yh", "x", "c", "z", "yl"))
    dp, expert = ("yh", "x", "c"), ("z", "yl")
    seqs, weights = P(dp, expert, None), P(expert, dp, None)
    return jax.shard_map(
        on_device,
        mesh=fine,
        in_specs=(seqs, seqs, P(), weights, weights),
        out_specs=(P(None, expert + dp, None), weights, weights),
        check_vma=False,
    )
```

```python
import functools

import jax
import jax.numpy as jnp
from jax import lax
from jax.experimental import pallas as pl
from jax.experimental.pallas import tpu as pltpu
from jax.sharding import Mesh
from jax.sharding import PartitionSpec as P

BF = jnp.bfloat16
F32 = jnp.float32
D = 4096
HALF = 2048
HID = 512
SEQS = 32
EXPERTS = 8
POS = 16
ROWS = SEQS * POS
LANES = EXPERTS * POS
SHARD = 256
MIB = 1024 * 1024
ORDER = (2, 1, 3, 0)
VM = pl.BlockSpec(memory_space=pltpu.VMEM)
HBM = pl.BlockSpec(memory_space=pltpu.HBM)


def call(kernel, outs, n_in, flops, nbytes, vmem, scratch=(), specs=None, far=0):
    return pl.pallas_call(
        kernel,
        out_shape=outs,
        in_specs=[VM] * n_in + [HBM] * far,
        out_specs=specs or jax.tree.map(lambda _: VM, outs),
        scratch_shapes=scratch,
        compiler_params=pltpu.CompilerParams(vmem_limit_bytes=vmem * MIB),
        cost_estimate=pl.CostEstimate(flops=flops, bytes_accessed=nbytes, transcendentals=0),
    )


def shape(dims, dtype):
    return jax.ShapeDtypeStruct(dims, dtype)


def in_hbm(x):
    return pltpu.with_memory_space_constraint(x, pltpu.HBM)


def nt(a, b):
    return lax.dot_general(a, b, (((1,), (1,)), ((), ())), preferred_element_type=F32)


def tn(a, b):
    return lax.dot_general(a, b, (((0,), (0,)), ((), ())), preferred_element_type=F32)


def pack_kernel(t_ref, g_ref, wi_ref, wo_ref, router_ref, o_ref, w_ref, rxt_ref, few, sem):
    copies = []
    for i in range(16):
        src, seq, part = (t_ref, g_ref)[i // 8], i // 4 % 2, pl.ds(i % 4 * 4, 4)
        copies.append(pltpu.make_async_copy(src.at[seq, part], o_ref.at[part, i // 4], sem.at[i]))
    copies.append(pltpu.make_async_copy(wi_ref.at[0], w_ref.at[0], sem.at[16]))
    copies.append(pltpu.make_async_copy(wo_ref.at[0], w_ref.at[1], sem.at[17]))
    scores = pltpu.make_async_copy(router_ref, few, sem.at[18])
    scores.start()
    for copy in copies:
        copy.start()
    scores.wait()
    for e in range(EXPERTS):
        row = few[e : e + 1, :].astype(F32)
        rxt_ref[e * POS : (e + 1) * POS, :] = jnp.broadcast_to(row, (POS, D)).astype(BF)
    for copy in copies:
        copy.wait()


def pack(tokens, out_grad, weight_in, weight_out, router):
    blocks = (2, 16, POS, D)
    arrays = (tokens.reshape(blocks), out_grad.reshape(blocks), weight_in, weight_out, router.T)
    return pl.pallas_call(
        pack_kernel,
        out_shape=(shape((16, 4, POS, D), BF), shape((2, SHARD, HID), BF), shape((LANES, D), BF)),
        in_specs=[HBM] * 5,
        out_specs=(VM, VM, VM),
        scratch_shapes=[pltpu.VMEM((EXPERTS, D), BF), pltpu.SemaphoreType.DMA((19,))],
        cost_estimate=pl.CostEstimate(flops=8 * MIB, bytes_accessed=16 * MIB, transcendentals=0),
        compiler_params=pltpu.CompilerParams(vmem_limit_bytes=16 * MIB),
        name="pack",
    )(*[in_hbm(a) for a in arrays])


def own_position():
    row = lax.broadcasted_iota(jnp.int32, (POS, LANES), 0)
    lane = lax.broadcasted_iota(jnp.int32, (POS, LANES), 1)
    return (lane % POS == row)[None]


def mix_kernel(a_ref, rxt_ref, f_ref, probs_ref, mixing_ref, held, sem):
    logits = jnp.zeros((LANES, ROWS), F32)
    for j in range(4):
        cols = pl.ds(j * 1024, 1024)
        logits += nt(rxt_ref[:, cols], a_ref[:, 0:2, :, cols].reshape(ROWS, 1024))
    logits = logits.T.reshape(SEQS, POS, LANES)
    weights = jnp.exp(logits - jnp.max(logits, axis=0, keepdims=True))
    probs = weights / jnp.sum(weights, axis=0, keepdims=True)
    probs = jnp.where(own_position(), probs, 0.0).reshape(ROWS, LANES)
    probs_ref[...] = probs
    mixing_ref[...] = probs.astype(BF)
    mixing_t = probs.T.astype(BF)
    copies = []
    for j in range(8):
        cols = pl.ds(j * 512, 512)
        half, part = j // 4, pl.ds(j % 4 * 512, 512)
        for t in range(2):
            block = a_ref[:, 2 * t : 2 * t + 2, :, cols].reshape(ROWS, 512)
            mixed = jnp.dot(mixing_t, block, preferred_element_type=F32)
            held[half, :, t, :, part] = mixed.astype(BF).reshape(EXPERTS, POS, 512)
        place = (half, slice(None), slice(None), slice(None), part)
        copies.append(pltpu.make_async_copy(held.at[place], f_ref.at[place], sem.at[j]))
        copies[j].start()
    for copy in copies:
        copy.wait()


def shard_columns(k, j):
    owner = lax.rem(lax.axis_index("x") + 4 - k, 4) * 2 + lax.rem(lax.axis_index("c") + j, 2)
    return pl.ds(pl.multiple_of(owner * SHARD, SHARD), SHARD)


def partial_kernel(t, f_ref, *refs):
    shard_refs, (own_ref, send_ref, w_ref, sem) = refs[:8], refs[8:]
    copies = [pltpu.make_async_copy(ref.at[t], w_ref.at[i], sem.at[i]) for i, ref in enumerate(shard_refs)]
    for copy in copies:
        copy.start()
    total = jnp.zeros((256, HID), F32)
    for i, copy in enumerate(copies):
        cols = shard_columns(i // 2, i % 2)
        copy.wait()
        block = f_ref[:, t, :, cols].reshape(256, SHARD)
        total += jnp.dot(block, w_ref[i], preferred_element_type=F32)
    own_ref[...] = total
    send_ref[...] = total.astype(BF)


def forward_kernel(own_ref, other_ref, w_ref, out_ref, pre_ref, hidden_ref):
    pre = own_ref[...] + other_ref[...].astype(F32)
    pre_ref[...] = pre
    hidden = (pre * jax.nn.sigmoid(pre)).astype(BF)
    hidden_ref[...] = hidden
    for i in range(8):
        cols = shard_columns(i // 2, i % 2)
        out_ref[:, :, cols] = nt(hidden, w_ref[i]).astype(BF).reshape(16, POS, SHARD)


def backward_kernel(own_ref, other_ref, pre_ref, w_ref, out_ref, b_ref, hidden_grad_ref, held, sem):
    copies = [pltpu.make_async_copy(out_ref, b_ref.at[:, 0], sem.at[2])]
    copies[0].start()
    pre = pre_ref[...]
    sigma = jax.nn.sigmoid(pre)
    hidden_full = own_ref[...] + other_ref[...].astype(F32)
    hidden_grad = (hidden_full * sigma * (1.0 + pre * (1.0 - sigma))).astype(BF)
    hidden_grad_ref[...] = hidden_grad
    for r in range(2):
        part = pl.ds(8 * r, 8)
        for i in range(8):
            block = nt(hidden_grad[128 * r : 128 * r + 128], w_ref[i])
            held[part, :, shard_columns(i // 2, i % 2)] = block.astype(BF).reshape(8, POS, SHARD)
        copies.append(pltpu.make_async_copy(held.at[part], b_ref.at[part, 1], sem.at[r]))
        copies[-1].start()
    for copy in copies:
        copy.wait()


def grads_kernel(f_ref, hidden_grad_ref, hidden_ref, *out_refs):
    for n, k in enumerate(ORDER):
        for j in range(2):
            cols = shard_columns(4 - k, j)
            for t, ref in enumerate((hidden_grad_ref, hidden_ref)):
                block = f_ref[:, t, :, cols].reshape(256, SHARD)
                out_refs[2 * n + j][t] = tn(block, ref[...]).astype(BF)


def add_kernel(keep_ref, got_ref, o_ref):
    o_ref[...] = (keep_ref[...].astype(F32) + got_ref[...].astype(F32)).astype(o_ref.dtype)


def sum_kernel(own_ref, a_ref, b_ref, c_ref, in_ref, out_ref):
    for t, ref in enumerate((in_ref, out_ref)):
        ref[0] = own_ref[t] + a_ref[t].astype(F32) + b_ref[t].astype(F32) + c_ref[t].astype(F32)


def final_kernel(b_ref, probs_ref, mixing_ref, rows_ref, far_rxt_ref, o_ref, a_ref, rxt_ref, held, in_sem, sem):
    reads = []
    for j in range(8):
        cols = pl.ds(j * 512, 512)
        reads.append(pltpu.make_async_copy(rows_ref.at[..., cols], a_ref.at[..., cols], in_sem.at[j]))
    reads.append(pltpu.make_async_copy(far_rxt_ref, rxt_ref, in_sem.at[8]))
    for copy in reads:
        copy.start()
    weight_grad = jnp.zeros((LANES, ROWS), F32)
    for j in range(8):
        cols = pl.ds(j * 512, 512)
        reads[j].wait()
        half, part = pl.ds(j // 4 * EXPERTS, EXPERTS), pl.ds(j % 4 * 512, 512)
        for t in range(2):
            block = a_ref[:, 2 - 2 * t : 4 - 2 * t, :, cols].reshape(ROWS, 512)
            weight_grad += nt(b_ref[half, t, :, part].reshape(LANES, 512), block)
    probs = probs_ref[...].reshape(SEQS, POS, LANES)
    weight_grad = weight_grad.T.reshape(SEQS, POS, LANES)
    mean = jnp.sum(probs * weight_grad, axis=0, keepdims=True)
    logit_grad = (probs * (weight_grad - mean)).reshape(ROWS, LANES).astype(BF)
    both = jnp.concatenate([mixing_ref[...], logit_grad], axis=1)
    reads[8].wait()
    copies = []
    for j in range(8):
        cols = pl.ds(j * 512, 512)
        half, part = pl.ds(j // 4 * EXPERTS, EXPERTS), pl.ds(j % 4 * 512, 512)
        right = jnp.concatenate([b_ref[half, 1, :, part].reshape(LANES, 512), rxt_ref[:, cols]], axis=0)
        out = jnp.dot(both, right, preferred_element_type=F32)
        held[:, :, cols] = out.astype(BF).reshape(SEQS, POS, 512)
        copies.append(pltpu.make_async_copy(held.at[:, :, cols], o_ref.at[:, :, cols], sem.at[j]))
        copies[j].start()
    for copy in copies:
        copy.wait()


def shift(x, k):
    return lax.ppermute(x, "x", [(i, (i + k) % 4) for i in range(4)])


def swap(x, axis):
    return lax.ppermute(x, axis, [(0, 1), (1, 0)])


def on_device(tokens, out_grad, router, weight_in, weight_out):
    rows, shard, rxt = pack(tokens, out_grad, weight_in, weight_out, router)
    rows = lax.all_to_all(rows, ("yh", "x", "c"), 0, 0, tiled=True)
    mixed, probs, mixing = call(
        mix_kernel,
        (pltpu.HBM((2, EXPERTS, 2, POS, HALF), BF), shape((ROWS, LANES), F32), shape((ROWS, LANES), BF)),
        2, 3 * 10**9, 12 * MIB, 22, specs=(HBM, VM, VM),
        scratch=[pltpu.VMEM((2, EXPERTS, 2, POS, HALF), BF), pltpu.SemaphoreType.DMA((8,))],
    )(rows, rxt)

    experts = ("yh", "z", "yl")
    got = lax.all_to_all(mixed.reshape(16, 2, POS, HALF), experts, 0, 0, tiled=True)

    shard, _ = lax.optimization_barrier((shard, mixing))
    shards = [shard] + [shift(shard, k) for k in range(1, 4)]
    weights = []
    for w in shards:
        weights += [w, swap(w, "c")]

    far_weights = [in_hbm(w) for w in weights]
    wide, narrow = shape((256, HID), F32), shape((256, HID), BF)
    owns, others, weights = [], [], []
    for t in range(2):
        own, send, w = call(
            functools.partial(partial_kernel, t), (wide, narrow, shape((8, SHARD, HID), BF)),
            1, 10**9, 4 * MIB, 10, far=8, scratch=[pltpu.SemaphoreType.DMA((8,))],
        )(got, *far_weights)
        owns.append(own)
        weights.append(w)
        others.append(swap(send, "yh"))
    out, pre, hidden = call(
        forward_kernel, (shape((16, POS, HALF), BF), wide, narrow), 3, 10**9, 4 * MIB, 10,
    )(owns[0], others[0], weights[1])
    back, hidden_grad = call(
        backward_kernel, (pltpu.HBM((16, 2, POS, HALF), BF), narrow),
        5, 10**9, 4 * MIB, 10, specs=(HBM, VM),
        scratch=[pltpu.VMEM((16, POS, HALF), BF), pltpu.SemaphoreType.DMA((3,))],
    )(owns[1], others[1], pre, weights[0], out)
    back = lax.all_to_all(back, experts, 0, 0, tiled=True)

    piece = shape((2, SHARD, HID), BF)
    parts = call(grads_kernel, (piece,) * 8, 3, 10**9, 8 * MIB, 14)(got, hidden_grad, hidden)
    sums = []
    for n, k in enumerate(ORDER):
        got_part = swap(parts[2 * n + 1], "c")
        total = shape((2, SHARD, HID), BF if k else F32)
        sums.append(call(add_kernel, total, 2, 10**6, 2 * MIB, 4)(parts[2 * n], got_part))
    sums = [shift(x, k) if k else x for x, k in zip(sums, ORDER)]
    token_grad = call(
        final_kernel, shape((SEQS, POS, D), BF), 3, 4 * 10**9, 16 * MIB, 32, specs=HBM, far=2,
        scratch=[
            pltpu.VMEM((16, 4, POS, D), BF),
            pltpu.VMEM((LANES, D), BF),
            pltpu.VMEM((SEQS, POS, D), BF),
            pltpu.SemaphoreType.DMA((9,)),
            pltpu.SemaphoreType.DMA((8,)),
        ],
    )(back, probs, mixing, in_hbm(rows), in_hbm(rxt))
    token_grad, *sums = lax.optimization_barrier((token_grad, *sums))
    grad = shape((1, SHARD, HID), F32)
    grad_in, grad_out = call(sum_kernel, (grad, grad), 4, 10**6, 4 * MIB, 6)(
        sums[3], sums[0], sums[1], sums[2]
    )
    return token_grad, grad_in, grad_out


def solution(mesh):
    fine = Mesh(mesh.devices.reshape(2, 4, 2, 4, 2), ("yh", "x", "c", "z", "yl"))
    dp, expert = ("yh", "x", "c"), ("z", "yl")
    seqs, weights = P(dp, expert, None), P(expert, dp, None)
    return jax.shard_map(
        on_device,
        mesh=fine,
        in_specs=(seqs, seqs, P(), weights, weights),
        out_specs=(P(None, expert + dp, None), weights, weights),
        check_vma=False,
    )
```

```python
import functools

import jax
import jax.numpy as jnp
from jax import lax
from jax.experimental import pallas as pl
from jax.experimental.pallas import tpu as pltpu
from jax.sharding import Mesh
from jax.sharding import PartitionSpec as P

BF = jnp.bfloat16
F32 = jnp.float32
D = 4096
HALF = 2048
HID = 512
SEQS = 32
EXPERTS = 8
POS = 16
ROWS = SEQS * POS
LANES = EXPERTS * POS
SHARD = 256
MIB = 1024 * 1024
ORDER = (2, 1, 3, 0)
VM = pl.BlockSpec(memory_space=pltpu.VMEM)
HBM = pl.BlockSpec(memory_space=pltpu.HBM)


def call(kernel, outs, n_in, flops, nbytes, vmem, scratch=(), specs=None, far=0):
    return pl.pallas_call(
        kernel,
        out_shape=outs,
        in_specs=[VM] * n_in + [HBM] * far,
        out_specs=specs or jax.tree.map(lambda _: VM, outs),
        scratch_shapes=scratch,
        compiler_params=pltpu.CompilerParams(vmem_limit_bytes=vmem * MIB),
        cost_estimate=pl.CostEstimate(flops=flops, bytes_accessed=nbytes, transcendentals=0),
    )


def shape(dims, dtype):
    return jax.ShapeDtypeStruct(dims, dtype)


def in_hbm(x):
    return pltpu.with_memory_space_constraint(x, pltpu.HBM)


def nt(a, b):
    return lax.dot_general(a, b, (((1,), (1,)), ((), ())), preferred_element_type=F32)


def tn(a, b):
    return lax.dot_general(a, b, (((0,), (0,)), ((), ())), preferred_element_type=F32)


def pack_kernel(t_ref, g_ref, wi_ref, wo_ref, router_ref, o_ref, w_ref, rxt_ref, few, sem):
    copies = []
    for i in range(16):
        src, seq, part = (t_ref, g_ref)[i // 8], i // 4 % 2, pl.ds(i % 4 * 4, 4)
        copies.append(pltpu.make_async_copy(src.at[seq, part], o_ref.at[part, i // 4], sem.at[i]))
    copies.append(pltpu.make_async_copy(wi_ref.at[0], w_ref.at[0], sem.at[16]))
    copies.append(pltpu.make_async_copy(wo_ref.at[0], w_ref.at[1], sem.at[17]))
    scores = pltpu.make_async_copy(router_ref, few, sem.at[18])
    scores.start()
    for copy in copies:
        copy.start()
    scores.wait()
    for e in range(EXPERTS):
        row = few[e : e + 1, :].astype(F32)
        rxt_ref[e * POS : (e + 1) * POS, :] = jnp.broadcast_to(row, (POS, D)).astype(BF)
    for copy in copies:
        copy.wait()


def pack(tokens, out_grad, weight_in, weight_out, router):
    blocks = (2, 16, POS, D)
    arrays = (tokens.reshape(blocks), out_grad.reshape(blocks), weight_in, weight_out, router.T)
    return pl.pallas_call(
        pack_kernel,
        out_shape=(shape((16, 4, POS, D), BF), shape((2, SHARD, HID), BF), shape((LANES, D), BF)),
        in_specs=[HBM] * 5,
        out_specs=(VM, VM, VM),
        scratch_shapes=[pltpu.VMEM((EXPERTS, D), BF), pltpu.SemaphoreType.DMA((19,))],
        cost_estimate=pl.CostEstimate(flops=8 * MIB, bytes_accessed=16 * MIB, transcendentals=0),
        compiler_params=pltpu.CompilerParams(vmem_limit_bytes=16 * MIB),
        name="pack",
    )(*[in_hbm(a) for a in arrays])


def own_position():
    row = lax.broadcasted_iota(jnp.int32, (POS, LANES), 0)
    lane = lax.broadcasted_iota(jnp.int32, (POS, LANES), 1)
    return (lane % POS == row)[None]


def mix_kernel(a_ref, rxt_ref, f_ref, probs_ref, mixing_ref, held, sem):
    logits = jnp.zeros((LANES, ROWS), F32)
    for j in range(4):
        cols = pl.ds(j * 1024, 1024)
        logits += nt(rxt_ref[:, cols], a_ref[:, 0:2, :, cols].reshape(ROWS, 1024))
    logits = logits.T.reshape(SEQS, POS, LANES)
    weights = jnp.exp(logits - jnp.max(logits, axis=0, keepdims=True))
    probs = weights / jnp.sum(weights, axis=0, keepdims=True)
    probs = jnp.where(own_position(), probs, 0.0).reshape(ROWS, LANES)
    probs_ref[...] = probs
    mixing_ref[...] = probs.astype(BF)
    mixing_t = probs.T.astype(BF)
    copies = []
    for j in range(8):
        cols = pl.ds(j * 512, 512)
        half, part = j // 4, pl.ds(j % 4 * 512, 512)
        for t in range(2):
            block = a_ref[:, 2 * t : 2 * t + 2, :, cols].reshape(ROWS, 512)
            mixed = jnp.dot(mixing_t, block, preferred_element_type=F32)
            held[:, half, t, :, part] = mixed.astype(BF).reshape(EXPERTS, POS, 512)
        if j % 4 == 3:
            place = (slice(None), half)
            copies.append(pltpu.make_async_copy(held.at[place], f_ref.at[place], sem.at[j]))
            copies[-1].start()
    for copy in copies:
        copy.wait()


def shard_columns(k, j):
    owner = lax.rem(lax.axis_index("x") + 4 - k, 4) * 2 + lax.rem(lax.axis_index("c") + j, 2)
    return pl.ds(pl.multiple_of(owner * SHARD, SHARD), SHARD)


def partial_kernel(t, f_ref, *refs):
    shard_refs, (own_ref, send_ref, w_ref, sem) = refs[:8], refs[8:]
    copies = [pltpu.make_async_copy(ref.at[t], w_ref.at[i], sem.at[i]) for i, ref in enumerate(shard_refs)]
    for copy in copies:
        copy.start()
    total = jnp.zeros((256, HID), F32)
    for i, copy in enumerate(copies):
        cols = shard_columns(i // 2, i % 2)
        copy.wait()
        block = f_ref[:, t, :, cols].reshape(256, SHARD)
        total += jnp.dot(block, w_ref[i], preferred_element_type=F32)
    own_ref[...] = total
    send_ref[...] = total.astype(BF)


def forward_kernel(own_ref, other_ref, w_ref, out_ref, pre_ref, hidden_ref):
    pre = own_ref[...] + other_ref[...].astype(F32)
    pre_ref[...] = pre
    hidden = (pre * jax.nn.sigmoid(pre)).astype(BF)
    hidden_ref[...] = hidden
    for i in range(8):
        cols = shard_columns(i // 2, i % 2)
        out_ref[:, :, cols] = nt(hidden, w_ref[i]).astype(BF).reshape(16, POS, SHARD)


def backward_kernel(own_ref, other_ref, pre_ref, w_ref, out_ref, b_ref, hidden_grad_ref, held, sem):
    copies = [pltpu.make_async_copy(out_ref, b_ref.at[:, 0], sem.at[2])]
    copies[0].start()
    pre = pre_ref[...]
    sigma = jax.nn.sigmoid(pre)
    hidden_full = own_ref[...] + other_ref[...].astype(F32)
    hidden_grad = (hidden_full * sigma * (1.0 + pre * (1.0 - sigma))).astype(BF)
    hidden_grad_ref[...] = hidden_grad
    for r in range(2):
        part = pl.ds(8 * r, 8)
        for i in range(8):
            block = nt(hidden_grad[128 * r : 128 * r + 128], w_ref[i])
            held[part, :, shard_columns(i // 2, i % 2)] = block.astype(BF).reshape(8, POS, SHARD)
        copies.append(pltpu.make_async_copy(held.at[part], b_ref.at[part, 1], sem.at[r]))
        copies[-1].start()
    for copy in copies:
        copy.wait()


def grads_kernel(f_ref, hidden_grad_ref, hidden_ref, *out_refs):
    for n, k in enumerate(ORDER):
        for j in range(2):
            cols = shard_columns(4 - k, j)
            for t, ref in enumerate((hidden_grad_ref, hidden_ref)):
                block = f_ref[:, t, :, cols].reshape(256, SHARD)
                out_refs[2 * n + j][t] = tn(block, ref[...]).astype(BF)


def add_kernel(keep_ref, got_ref, *o_refs):
    for t, o_ref in enumerate(o_refs):
        o_ref[...] = (keep_ref[t].astype(F32) + got_ref[t].astype(F32)).astype(o_ref.dtype)


def sum_kernel(own_ref, a_ref, b_ref, c_ref, o_ref):
    o_ref[0] = own_ref[...] + a_ref[...].astype(F32) + b_ref[...].astype(F32) + c_ref[...].astype(F32)


def final_kernel(b_ref, probs_ref, mixing_ref, rows_ref, far_rxt_ref, o_ref, a_ref, rxt_ref, held, in_sem, sem):
    reads = []
    for j in range(8):
        cols = pl.ds(j * 512, 512)
        reads.append(pltpu.make_async_copy(rows_ref.at[..., cols], a_ref.at[..., cols], in_sem.at[j]))
    reads.append(pltpu.make_async_copy(far_rxt_ref, rxt_ref, in_sem.at[8]))
    for copy in reads:
        copy.start()
    weight_grad = jnp.zeros((LANES, ROWS), F32)
    for j in range(8):
        cols = pl.ds(j * 512, 512)
        reads[j].wait()
        half, part = j // 4, pl.ds(j % 4 * 512, 512)
        for t in range(2):
            block = a_ref[:, 2 - 2 * t : 4 - 2 * t, :, cols].reshape(ROWS, 512)
            weight_grad += nt(b_ref[:, half, t, :, part].reshape(LANES, 512), block)
    probs = probs_ref[...].reshape(SEQS, POS, LANES)
    weight_grad = weight_grad.T.reshape(SEQS, POS, LANES)
    mean = jnp.sum(probs * weight_grad, axis=0, keepdims=True)
    logit_grad = (probs * (weight_grad - mean)).reshape(ROWS, LANES).astype(BF)
    both = jnp.concatenate([mixing_ref[...], logit_grad], axis=1)
    reads[8].wait()
    copies = []
    for j in range(8):
        cols = pl.ds(j * 512, 512)
        half, part = j // 4, pl.ds(j % 4 * 512, 512)
        right = jnp.concatenate([b_ref[:, half, 1, :, part].reshape(LANES, 512), rxt_ref[:, cols]], axis=0)
        out = jnp.dot(both, right, preferred_element_type=F32)
        held[:, :, cols] = out.astype(BF).reshape(SEQS, POS, 512)
        copies.append(pltpu.make_async_copy(held.at[:, :, cols], o_ref.at[:, :, cols], sem.at[j]))
        copies[j].start()
    for copy in copies:
        copy.wait()


def shift(x, k):
    return lax.ppermute(x, "x", [(i, (i + k) % 4) for i in range(4)])


def swap(x, axis):
    return lax.ppermute(x, axis, [(0, 1), (1, 0)])


def on_device(tokens, out_grad, router, weight_in, weight_out):
    rows, shard, rxt = pack(tokens, out_grad, weight_in, weight_out, router)
    rows = lax.all_to_all(rows, ("yh", "x", "c"), 0, 0, tiled=True)
    mixed, probs, mixing = call(
        mix_kernel,
        (pltpu.HBM((EXPERTS, 2, 2, POS, HALF), BF), shape((ROWS, LANES), F32), shape((ROWS, LANES), BF)),
        2, 3 * 10**9, 12 * MIB, 22, specs=(HBM, VM, VM),
        scratch=[pltpu.VMEM((EXPERTS, 2, 2, POS, HALF), BF), pltpu.SemaphoreType.DMA((8,))],
    )(rows, rxt)

    experts = ("z", "yl", "yh")
    got = lax.all_to_all(mixed.reshape(16, 2, POS, HALF), experts, 0, 0, tiled=True)

    shard, _ = lax.optimization_barrier((shard, mixing))
    shards = [shard] + [shift(shard, k) for k in range(1, 4)]
    weights = []
    for w in shards:
        weights += [w, swap(w, "c")]

    far_weights = [in_hbm(w) for w in weights]
    wide, narrow = shape((256, HID), F32), shape((256, HID), BF)
    owns, others, weights = [], [], []
    for t in range(2):
        own, send, w = call(
            functools.partial(partial_kernel, t), (wide, narrow, shape((8, SHARD, HID), BF)),
            1, 10**9, 4 * MIB, 10, far=8, scratch=[pltpu.SemaphoreType.DMA((8,))],
        )(got, *far_weights)
        owns.append(own)
        weights.append(w)
        others.append(swap(send, "yh"))
    out, pre, hidden = call(
        forward_kernel, (shape((16, POS, HALF), BF), wide, narrow), 3, 10**9, 4 * MIB, 10,
    )(owns[0], others[0], weights[1])
    back, hidden_grad = call(
        backward_kernel, (pltpu.HBM((16, 2, POS, HALF), BF), narrow),
        5, 10**9, 4 * MIB, 10, specs=(HBM, VM),
        scratch=[pltpu.VMEM((16, POS, HALF), BF), pltpu.SemaphoreType.DMA((3,))],
    )(owns[1], others[1], pre, weights[0], out)
    back = lax.all_to_all(back, experts, 0, 0, tiled=True)

    piece = shape((2, SHARD, HID), BF)
    parts = call(grads_kernel, (piece,) * 8, 3, 10**9, 8 * MIB, 14)(got, hidden_grad, hidden)
    sums = []
    for n, k in enumerate(ORDER):
        got_part = swap(parts[2 * n + 1], "c")
        total = shape((SHARD, HID), BF if k else F32)
        sums.append(call(add_kernel, (total, total), 2, 10**6, 2 * MIB, 4)(parts[2 * n], got_part))

    def group_sum(t, after):
        terms = lax.optimization_barrier(tuple(x[t] for x in sums) + after)[:4]
        terms = [shift(x, k) if k else x for x, k in zip(terms, ORDER)]
        return terms, call(sum_kernel, shape((1, SHARD, HID), F32), 4, 10**6, 4 * MIB, 4)

    terms, add_up = group_sum(1, ())
    grad_out = add_up(terms[3], *terms[:3])
    terms, add_up = group_sum(0, ())
    token_grad = call(
        final_kernel, shape((SEQS, POS, D), BF), 3, 4 * 10**9, 16 * MIB, 32, specs=HBM, far=2,
        scratch=[
            pltpu.VMEM((16, 4, POS, D), BF),
            pltpu.VMEM((LANES, D), BF),
            pltpu.VMEM((SEQS, POS, D), BF),
            pltpu.SemaphoreType.DMA((9,)),
            pltpu.SemaphoreType.DMA((8,)),
        ],
    )(back.reshape(EXPERTS, 2, 2, POS, HALF), probs, mixing, in_hbm(rows), in_hbm(rxt))
    token_grad, *terms = lax.optimization_barrier((token_grad, *terms))
    grad_in = add_up(terms[3], *terms[:3])
    return token_grad, grad_in, grad_out


def solution(mesh):
    fine = Mesh(mesh.devices.reshape(2, 4, 2, 4, 2), ("yh", "x", "c", "z", "yl"))
    dp, expert = ("yh", "x", "c"), ("z", "yl")
    seqs, weights = P(dp, expert, None), P(expert, dp, None)
    return jax.shard_map(
        on_device,
        mesh=fine,
        in_specs=(seqs, seqs, P(), weights, weights),
        out_specs=(P(None, expert + dp, None), weights, weights),
        check_vma=False,
    )
```

```python
import functools

import jax
import jax.numpy as jnp
from jax import lax
from jax.experimental import pallas as pl
from jax.experimental.pallas import tpu as pltpu
from jax.sharding import Mesh
from jax.sharding import PartitionSpec as P

BF = jnp.bfloat16
F32 = jnp.float32
D = 4096
HALF = 2048
HID = 512
SEQS = 32
EXPERTS = 8
POS = 16
ROWS = SEQS * POS
LANES = EXPERTS * POS
SHARD = 256
MIB = 1024 * 1024
ORDER = (2, 1, 3, 0)
VM = pl.BlockSpec(memory_space=pltpu.VMEM)
HBM = pl.BlockSpec(memory_space=pltpu.HBM)


def call(kernel, outs, n_in, flops, nbytes, vmem, scratch=(), specs=None, far=0):
    return pl.pallas_call(
        kernel,
        out_shape=outs,
        in_specs=[VM] * n_in + [HBM] * far,
        out_specs=specs or jax.tree.map(lambda _: VM, outs),
        scratch_shapes=scratch,
        compiler_params=pltpu.CompilerParams(vmem_limit_bytes=vmem * MIB),
        cost_estimate=pl.CostEstimate(flops=flops, bytes_accessed=nbytes, transcendentals=0),
    )


def shape(dims, dtype):
    return jax.ShapeDtypeStruct(dims, dtype)


def in_hbm(x):
    return pltpu.with_memory_space_constraint(x, pltpu.HBM)


def nt(a, b):
    return lax.dot_general(a, b, (((1,), (1,)), ((), ())), preferred_element_type=F32)


def tn(a, b):
    return lax.dot_general(a, b, (((0,), (0,)), ((), ())), preferred_element_type=F32)


def pack_kernel(t_ref, g_ref, wi_ref, wo_ref, router_ref, o_ref, w_ref, rxt_ref, few, sem):
    copies = []
    for i in range(16):
        src, seq, part = (t_ref, g_ref)[i // 8], i // 4 % 2, pl.ds(i % 4 * 4, 4)
        copies.append(pltpu.make_async_copy(src.at[seq, part], o_ref.at[part, i // 4], sem.at[i]))
    copies.append(pltpu.make_async_copy(wi_ref.at[0], w_ref.at[0], sem.at[16]))
    copies.append(pltpu.make_async_copy(wo_ref.at[0], w_ref.at[1], sem.at[17]))
    scores = pltpu.make_async_copy(router_ref, few, sem.at[18])
    scores.start()
    for copy in copies:
        copy.start()
    scores.wait()
    for e in range(EXPERTS):
        row = few[e : e + 1, :].astype(F32)
        rxt_ref[e * POS : (e + 1) * POS, :] = jnp.broadcast_to(row, (POS, D)).astype(BF)
    for copy in copies:
        copy.wait()


def pack(tokens, out_grad, weight_in, weight_out, router):
    blocks = (2, 16, POS, D)
    arrays = (tokens.reshape(blocks), out_grad.reshape(blocks), weight_in, weight_out, router.T)
    return pl.pallas_call(
        pack_kernel,
        out_shape=(shape((16, 4, POS, D), BF), shape((2, SHARD, HID), BF), shape((LANES, D), BF)),
        in_specs=[HBM] * 5,
        out_specs=(VM, VM, VM),
        scratch_shapes=[pltpu.VMEM((EXPERTS, D), BF), pltpu.SemaphoreType.DMA((19,))],
        cost_estimate=pl.CostEstimate(flops=8 * MIB, bytes_accessed=16 * MIB, transcendentals=0),
        compiler_params=pltpu.CompilerParams(vmem_limit_bytes=16 * MIB),
        name="pack",
    )(*[in_hbm(a) for a in arrays])


def own_position():
    row = lax.broadcasted_iota(jnp.int32, (POS, LANES), 0)
    lane = lax.broadcasted_iota(jnp.int32, (POS, LANES), 1)
    return (lane % POS == row)[None]


def mix_kernel(a_ref, rxt_ref, f_ref, probs_ref, mixing_ref, held, sem):
    logits = jnp.zeros((LANES, ROWS), F32)
    for j in range(4):
        cols = pl.ds(j * 1024, 1024)
        logits += nt(rxt_ref[:, cols], a_ref[:, 0:2, :, cols].reshape(ROWS, 1024))
    logits = logits.T.reshape(SEQS, POS, LANES)
    weights = jnp.exp(logits - jnp.max(logits, axis=0, keepdims=True))
    probs = weights / jnp.sum(weights, axis=0, keepdims=True)
    probs = jnp.where(own_position(), probs, 0.0).reshape(ROWS, LANES)
    probs_ref[...] = probs
    mixing_ref[...] = probs.astype(BF)
    mixing_t = probs.T.astype(BF)
    copies = []
    for j in range(8):
        cols = pl.ds(j * 512, 512)
        half, part = j // 4, pl.ds(j % 4 * 512, 512)
        for t in range(2):
            block = a_ref[:, 2 * t : 2 * t + 2, :, cols].reshape(ROWS, 512)
            mixed = jnp.dot(mixing_t, block, preferred_element_type=F32)
            held[:, half, t, :, part] = mixed.astype(BF).reshape(EXPERTS, POS, 512)
        if j in (3, 5, 7):
            first = max(j - 5, 0) * 512
            place = (slice(None), half, slice(None), slice(None), pl.ds(first, HALF if j == 3 else 1024))
            copies.append(pltpu.make_async_copy(held.at[place], f_ref.at[place], sem.at[j]))
            copies[-1].start()
    for copy in copies:
        copy.wait()


def shard_columns(k, j):
    owner = lax.rem(lax.axis_index("x") + 4 - k, 4) * 2 + lax.rem(lax.axis_index("c") + j, 2)
    return pl.ds(pl.multiple_of(owner * SHARD, SHARD), SHARD)


def partial_kernel(t, f_ref, *refs):
    shard_refs, (own_ref, send_ref, w_ref, sem) = refs[:8], refs[8:]
    copies = [pltpu.make_async_copy(ref.at[t], w_ref.at[i], sem.at[i]) for i, ref in enumerate(shard_refs)]
    for copy in copies:
        copy.start()
    total = jnp.zeros((256, HID), F32)
    for i, copy in enumerate(copies):
        cols = shard_columns(i // 2, i % 2)
        copy.wait()
        block = f_ref[:, t, :, cols].reshape(256, SHARD)
        total += jnp.dot(block, w_ref[i], preferred_element_type=F32)
    own_ref[...] = total
    send_ref[...] = total.astype(BF)


def forward_kernel(own_ref, other_ref, w_ref, out_ref, pre_ref, hidden_ref):
    pre = own_ref[...] + other_ref[...].astype(F32)
    pre_ref[...] = pre
    hidden = (pre * jax.nn.sigmoid(pre)).astype(BF)
    hidden_ref[...] = hidden
    for i in range(8):
        cols = shard_columns(i // 2, i % 2)
        out_ref[:, :, cols] = nt(hidden, w_ref[i]).astype(BF).reshape(16, POS, SHARD)


def backward_kernel(own_ref, other_ref, pre_ref, w_ref, out_ref, b_ref, hidden_grad_ref, held, sem):
    copies = [pltpu.make_async_copy(out_ref, b_ref.at[:, 0], sem.at[2])]
    copies[0].start()
    pre = pre_ref[...]
    sigma = jax.nn.sigmoid(pre)
    hidden_full = own_ref[...] + other_ref[...].astype(F32)
    hidden_grad = (hidden_full * sigma * (1.0 + pre * (1.0 - sigma))).astype(BF)
    hidden_grad_ref[...] = hidden_grad
    for r in range(2):
        part = pl.ds(8 * r, 8)
        for i in range(8):
            block = nt(hidden_grad[128 * r : 128 * r + 128], w_ref[i])
            held[part, :, shard_columns(i // 2, i % 2)] = block.astype(BF).reshape(8, POS, SHARD)
        copies.append(pltpu.make_async_copy(held.at[part], b_ref.at[part, 1], sem.at[r]))
        copies[-1].start()
    for copy in copies:
        copy.wait()


def grads_kernel(f_ref, hidden_grad_ref, hidden_ref, *out_refs):
    for n, k in enumerate(ORDER):
        for j in range(2):
            cols = shard_columns(4 - k, j)
            for t, ref in enumerate((hidden_grad_ref, hidden_ref)):
                block = f_ref[:, t, :, cols].reshape(256, SHARD)
                out_refs[2 * n + j][t] = tn(block, ref[...]).astype(BF)


def add_kernel(keep_ref, got_ref, *o_refs):
    for t, o_ref in enumerate(o_refs):
        o_ref[...] = (keep_ref[t].astype(F32) + got_ref[t].astype(F32)).astype(o_ref.dtype)


def sum_kernel(own_ref, a_ref, b_ref, c_ref, o_ref):
    o_ref[0] = own_ref[...] + a_ref[...].astype(F32) + b_ref[...].astype(F32) + c_ref[...].astype(F32)


def final_kernel(b_ref, probs_ref, mixing_ref, rows_ref, far_rxt_ref, o_ref, a_ref, rxt_ref, held, in_sem, sem):
    reads = []
    for j in range(8):
        cols = pl.ds(j * 512, 512)
        reads.append(pltpu.make_async_copy(rows_ref.at[..., cols], a_ref.at[..., cols], in_sem.at[j]))
    reads.append(pltpu.make_async_copy(far_rxt_ref, rxt_ref, in_sem.at[8]))
    for copy in reads:
        copy.start()
    weight_grad = jnp.zeros((LANES, ROWS), F32)
    for j in range(8):
        cols = pl.ds(j * 512, 512)
        reads[j].wait()
        half, part = j // 4, pl.ds(j % 4 * 512, 512)
        for t in range(2):
            block = a_ref[:, 2 - 2 * t : 4 - 2 * t, :, cols].reshape(ROWS, 512)
            weight_grad += nt(b_ref[:, half, t, :, part].reshape(LANES, 512), block)
    probs = probs_ref[...].reshape(SEQS, POS, LANES)
    weight_grad = weight_grad.T.reshape(SEQS, POS, LANES)
    mean = jnp.sum(probs * weight_grad, axis=0, keepdims=True)
    logit_grad = (probs * (weight_grad - mean)).reshape(ROWS, LANES).astype(BF)
    both = jnp.concatenate([mixing_ref[...], logit_grad], axis=1)
    reads[8].wait()
    copies = []
    for j in range(8):
        cols = pl.ds(j * 512, 512)
        half, part = j // 4, pl.ds(j % 4 * 512, 512)
        right = jnp.concatenate([b_ref[:, half, 1, :, part].reshape(LANES, 512), rxt_ref[:, cols]], axis=0)
        out = jnp.dot(both, right, preferred_element_type=F32)
        held[:, :, cols] = out.astype(BF).reshape(SEQS, POS, 512)
        copies.append(pltpu.make_async_copy(held.at[:, :, cols], o_ref.at[:, :, cols], sem.at[j]))
        copies[j].start()
    for copy in copies:
        copy.wait()


def shift(x, k):
    return lax.ppermute(x, "x", [(i, (i + k) % 4) for i in range(4)])


def swap(x, axis):
    return lax.ppermute(x, axis, [(0, 1), (1, 0)])


def on_device(tokens, out_grad, router, weight_in, weight_out):
    rows, shard, rxt = pack(tokens, out_grad, weight_in, weight_out, router)
    rows = lax.all_to_all(rows, ("yh", "x", "c"), 0, 0, tiled=True)
    mixed, probs, mixing = call(
        mix_kernel,
        (pltpu.HBM((EXPERTS, 2, 2, POS, HALF), BF), shape((ROWS, LANES), F32), shape((ROWS, LANES), BF)),
        2, 3 * 10**9, 12 * MIB, 22, specs=(HBM, VM, VM),
        scratch=[pltpu.VMEM((EXPERTS, 2, 2, POS, HALF), BF), pltpu.SemaphoreType.DMA((8,))],
    )(rows, rxt)

    experts = ("z", "yl", "yh")
    got = lax.all_to_all(mixed.reshape(16, 2, POS, HALF), experts, 0, 0, tiled=True)

    shard, _ = lax.optimization_barrier((shard, mixing))
    shards = [shard] + [shift(shard, k) for k in range(1, 4)]
    weights = []
    for w in shards:
        weights += [w, swap(w, "c")]

    far_weights = [in_hbm(w) for w in weights]
    wide, narrow = shape((256, HID), F32), shape((256, HID), BF)
    owns, others, weights = [], [], []
    for t in range(2):
        own, send, w = call(
            functools.partial(partial_kernel, t), (wide, narrow, shape((8, SHARD, HID), BF)),
            1, 10**9, 4 * MIB, 10, far=8, scratch=[pltpu.SemaphoreType.DMA((8,))],
        )(got, *far_weights)
        owns.append(own)
        weights.append(w)
        others.append(swap(send, "yh"))
    out, pre, hidden = call(
        forward_kernel, (shape((16, POS, HALF), BF), wide, narrow), 3, 10**9, 4 * MIB, 10,
    )(owns[0], others[0], weights[1])
    back, hidden_grad = call(
        backward_kernel, (pltpu.HBM((16, 2, POS, HALF), BF), narrow),
        5, 10**9, 4 * MIB, 10, specs=(HBM, VM),
        scratch=[pltpu.VMEM((16, POS, HALF), BF), pltpu.SemaphoreType.DMA((3,))],
    )(owns[1], others[1], pre, weights[0], out)
    back = lax.all_to_all(back, experts, 0, 0, tiled=True)

    piece = shape((2, SHARD, HID), BF)
    parts = call(grads_kernel, (piece,) * 8, 3, 10**9, 8 * MIB, 14)(got, hidden_grad, hidden)
    sums = []
    for n, k in enumerate(ORDER):
        got_part = swap(parts[2 * n + 1], "c")
        total = shape((SHARD, HID), BF if k else F32)
        sums.append(call(add_kernel, (total, total), 2, 10**6, 2 * MIB, 4)(parts[2 * n], got_part))

    def group_sum(t, after):
        terms = lax.optimization_barrier(tuple(x[t] for x in sums) + after)[:4]
        terms = [shift(x, k) if k else x for x, k in zip(terms, ORDER)]
        return terms, call(sum_kernel, shape((1, SHARD, HID), F32), 4, 10**6, 4 * MIB, 4)

    terms, add_up = group_sum(1, ())
    grad_out = add_up(terms[3], *terms[:3])
    terms, add_up = group_sum(0, ())
    token_grad = call(
        final_kernel, shape((SEQS, POS, D), BF), 3, 4 * 10**9, 16 * MIB, 32, specs=HBM, far=2,
        scratch=[
            pltpu.VMEM((16, 4, POS, D), BF),
            pltpu.VMEM((LANES, D), BF),
            pltpu.VMEM((SEQS, POS, D), BF),
            pltpu.SemaphoreType.DMA((9,)),
            pltpu.SemaphoreType.DMA((8,)),
        ],
    )(back.reshape(EXPERTS, 2, 2, POS, HALF), probs, mixing, in_hbm(rows), in_hbm(rxt))
    token_grad, *terms = lax.optimization_barrier((token_grad, *terms))
    grad_in = add_up(terms[3], *terms[:3])
    return token_grad, grad_in, grad_out


def solution(mesh):
    fine = Mesh(mesh.devices.reshape(2, 4, 2, 4, 2), ("yh", "x", "c", "z", "yl"))
    dp, expert = ("yh", "x", "c"), ("z", "yl")
    seqs, weights = P(dp, expert, None), P(expert, dp, None)
    return jax.shard_map(
        on_device,
        mesh=fine,
        in_specs=(seqs, seqs, P(), weights, weights),
        out_specs=(P(None, expert + dp, None), weights, weights),
        check_vma=False,
    )
```
